64 devices in a mesh: dp: 4 (over x, y), tp: 16 (over z, core).
Axes of the slice: x: 2, y: 2, z: 8, core: 2. Of those that a mesh axis runs over, the one named last changes fastest.
The devices are a block of a 4x4x8 slice.
Arguments:
- enc_out: bfloat16 [4, 2048, 4096], P('dp', 'tp'), parts along dimension 0
- norm_scale: bfloat16 [4096], replicated
- w_key: bfloat16 [6, 4096, 16, 256], P(None, None, 'tp')
- w_value: bfloat16 [6, 4096, 16, 256], P(None, None, 'tp')
Outputs:
- output 1: bfloat16 [6, 4, 2048, 16, 256], P(None, 'dp', None, 'tp'), parts along dimension 1
- output 2: bfloat16 [6, 4, 2048, 16, 256], P(None, 'dp', None, 'tp'), parts along dimension 1
There are 4 independent parts. The reference program is written for one: setup_inputs(seed, part) draws one part's arguments, and reference() takes and returns one part's arrays. A program takes and returns all parts, laid end to end along the dimension named above; an argument that names none is the same for every part.
All inputs are finite; a program needn't handle non-finite values.
Results may differ from the reference program's by a relative error of at most 0.001.
Values are sent between devices in bfloat16 or wider.
A program may use at most 768 MiB of HBM per device.

```python
import jax
import jax.numpy as jnp
from jax import lax

N_LAYERS = 6
BATCH_SIZE = 1
SEQ_LEN = 2048
D_MODEL = 4096
N_HEADS = 16
HEAD_DIM = 256
NORM_EPS = 1e-6


def setup_inputs(seed: int = 0, part: int = 0) -> dict:
    root_key = jax.random.key(seed)
    k_act, k_norm, k_key, k_val = jax.random.split(root_key, 4)
    k_act = jax.random.fold_in(k_act, part)
    w_scale = D_MODEL ** -0.5
    w_shape = (N_LAYERS, D_MODEL, N_HEADS, HEAD_DIM)
    enc_out = jax.random.normal(k_act, (BATCH_SIZE, SEQ_LEN, D_MODEL), jnp.float32)
    norm_scale = jax.random.uniform(k_norm, (D_MODEL,), jnp.float32, 0.5, 1.5)
    w_key = jax.random.normal(k_key, w_shape, jnp.float32) * w_scale
    w_value = jax.random.normal(k_val, w_shape, jnp.float32) * w_scale
    return {"enc_out": enc_out.astype(jnp.bfloat16), "norm_scale": norm_scale.astype(jnp.bfloat16), "w_key": w_key.astype(jnp.bfloat16), "w_value": w_value.astype(jnp.bfloat16)}


def rms_norm(enc_out, norm_scale):
    acts = enc_out.astype(jnp.float32)
    mean_sq = jnp.mean(acts * acts, axis=-1, keepdims=True)
    return (acts * lax.rsqrt(mean_sq + NORM_EPS) * norm_scale.astype(jnp.float32)).astype(jnp.bfloat16)


def reference(enc_out, norm_scale, w_key, w_value):
    normed = rms_norm(enc_out, norm_scale).reshape(BATCH_SIZE * SEQ_LEN, D_MODEL)
    out_shape = (BATCH_SIZE, SEQ_LEN, N_HEADS, HEAD_DIM)

    def project(layer_weights):
        layer_key, layer_value = layer_weights
        keys = jnp.dot(normed, layer_key.reshape(D_MODEL, N_HEADS * HEAD_DIM), preferred_element_type=jnp.float32)
        values = jnp.dot(normed, layer_value.reshape(D_MODEL, N_HEADS * HEAD_DIM), preferred_element_type=jnp.float32)
        return keys.astype(jnp.bfloat16).reshape(out_shape), values.astype(jnp.bfloat16).reshape(out_shape)

    key_cache, value_cache = lax.map(project, (w_key, w_value))
    return key_cache, value_cache
```

```python
import functools

import jax
import jax.numpy as jnp
from jax import lax
from jax.experimental import pallas as pl
from jax.experimental.pallas import tpu as pltpu
from jax.sharding import PartitionSpec as P

NORM_EPS = 1e-6
MESH = pl.DeviceIdType.MESH
NORM_ROWS = 32


def ring_body(n, x_hbm, scale_ref, wk_hbm, wv_hbm, out, acts, tokens, weights, in_sem, w_sem, cw_send, cw_recv, ccw_send, ccw_recv, mate_send, mate_recv):
    me = lax.axis_index("tp")
    mate = me + 1 - 2 * lax.rem(me, 2)
    after = lax.rem(me + 2, n)
    before = lax.rem(me + n - 2, n)
    block, d_model = acts.shape
    half = block // 2
    n_layers, _, both = weights.shape
    head_dim = both // 2
    hops = n // 2 - 1

    x_copy = pltpu.make_async_copy(x_hbm, acts, in_sem)
    x_copy.start()
    w_copies = []
    for layer in range(n_layers):
        w_copies.append((
            pltpu.make_async_copy(wk_hbm.at[layer], weights.at[layer, :, pl.ds(0, head_dim)], w_sem.at[2 * layer]),
            pltpu.make_async_copy(wv_hbm.at[layer], weights.at[layer, :, pl.ds(head_dim, head_dim)], w_sem.at[2 * layer + 1]),
        ))

    barrier = pltpu.get_barrier_semaphore()
    for other in (after, before, mate):
        pl.semaphore_signal(barrier, inc=1, device_id={"tp": other}, device_id_type=MESH)

    scale = scale_ref[...].astype(jnp.float32)
    x_copy.wait()
    for pair in w_copies:
        for copy in pair:
            copy.start()

    def normalize(start):
        @pl.loop(0, half // NORM_ROWS)
        def _(i):
            rows = pl.ds(pl.multiple_of(start + i * NORM_ROWS, NORM_ROWS), NORM_ROWS)
            x = acts[rows, :].astype(jnp.float32)
            mean_sq = jnp.mean(x * x, axis=-1, keepdims=True)
            tokens[0, rows, :] = (x * lax.rsqrt(mean_sq + NORM_EPS) * scale).astype(jnp.bfloat16)

    normalize(0)
    normalize(half)
    pl.semaphore_wait(barrier, 3)

    sends = []

    def send(src, dst, send_sem, recv_sem, other):
        copy = pltpu.make_async_remote_copy(src_ref=src, dst_ref=dst, send_sem=send_sem, recv_sem=recv_sem, device_id={"tp": other}, device_id_type=MESH)
        copy.start()
        sends.append(copy)
        return copy

    def send_ring(slot, forward):
        if forward:
            src = tokens.at[0, pl.ds(half * slot, half)] if slot < 2 else tokens.at[slot - 1, pl.ds(0, half)]
            return send(src, tokens.at[slot + 1, pl.ds(0, half)], cw_send.at[slot], cw_recv.at[slot], after)
        src = tokens.at[0, pl.ds(half * (1 - slot), half)] if slot < 2 else tokens.at[slot - 1, pl.ds(half, half)]
        return send(src, tokens.at[slot + 1, pl.ds(half, half)], ccw_send.at[slot], ccw_recv.at[slot], before)

    def send_mate(step):
        return send(tokens.at[step, pl.ds(0, block)], tokens.at[step, pl.ds(block, block)], mate_send.at[step], mate_recv.at[step], mate)

    def project(step, first):
        @pl.loop(0, n_layers)
        def _(layer):
            if first:
                for side in range(2):
                    pltpu.make_async_copy(wk_hbm.at[layer], weights.at[layer, :, pl.ds(side * head_dim, head_dim)], w_sem.at[2 * layer + side]).wait()
            out[step, layer] = jnp.dot(tokens[step], weights[layer], preferred_element_type=jnp.float32).astype(jnp.bfloat16)

    ring = {}
    for slot in range(2):
        ring[slot] = (send_ring(slot, True), send_ring(slot, False))
    swap = send_mate(0)
    swap.wait_recv()
    project(0, True)
    for slot in range(hops):
        for copy in ring[slot]:
            copy.wait_recv()
        if slot + 2 < hops:
            ring[slot + 2] = (send_ring(slot + 2, True), send_ring(slot + 2, False))
        swap = send_mate(slot + 1)
        swap.wait_recv()
        project(slot + 1, False)
    for copy in sends:
        copy.wait_send()


def place_body(n, block, res, k_hbm, v_hbm, sem):
    me = lax.axis_index("tp")
    mate = me + 1 - 2 * lax.rem(me, 2)
    half = block // 2
    steps, _, _, both = res.shape
    head_dim = both // 2
    copies = []
    for step in range(steps):
        for group in range(4):
            who = me if group < 2 else mate
            if step == 0:
                start = who * block + (group % 2) * half
            else:
                slot = step - 1
                away = 2 + 2 * (slot // 2)
                if group % 2 == 0:
                    start = lax.rem(who + n - away, n) * block + (slot % 2) * half
                else:
                    start = lax.rem(who + away, n) * block + ((slot + 1) % 2) * half
            rows = pl.ds(pl.multiple_of(start, half), half)
            for side, dst in enumerate((k_hbm, v_hbm)):
                copy = pltpu.make_async_copy(res.at[step, :, pl.ds(group * half, half), pl.ds(side * head_dim, head_dim)], dst.at[:, rows, :], sem.at[len(copies)])
                copy.start()
                copies.append(copy)
    for copy in copies:
        copy.wait()


def solution(mesh):
    n = mesh.shape["tp"]

    def per_device(enc_out, norm_scale, w_key, w_value):
        _, block, d_model = enc_out.shape
        n_layers, _, _, head_dim = w_key.shape
        hops = n // 2 - 1
        anywhere = pl.BlockSpec(memory_space=pl.ANY)
        in_vmem = pl.BlockSpec(memory_space=pltpu.VMEM)
        res = pl.pallas_call(
            functools.partial(ring_body, n),
            out_shape=pltpu.VMEM((hops + 1, n_layers, 2 * block, 2 * head_dim), jnp.bfloat16),
            in_specs=[anywhere, in_vmem, anywhere, anywhere],
            out_specs=in_vmem,
            scratch_shapes=[
                pltpu.VMEM((block, d_model), jnp.bfloat16),
                pltpu.VMEM((hops + 1, 2 * block, d_model), jnp.bfloat16),
                pltpu.VMEM((n_layers, d_model, 2 * head_dim), jnp.bfloat16),
                pltpu.SemaphoreType.DMA,
                pltpu.SemaphoreType.DMA((2 * n_layers,)),
                pltpu.SemaphoreType.DMA((hops,)),
                pltpu.SemaphoreType.DMA((hops,)),
                pltpu.SemaphoreType.DMA((hops,)),
                pltpu.SemaphoreType.DMA((hops,)),
                pltpu.SemaphoreType.DMA((hops + 1,)),
                pltpu.SemaphoreType.DMA((hops + 1,)),
            ],
            compiler_params=pltpu.CompilerParams(collective_id=0, has_side_effects=True, vmem_limit_bytes=48 * 1024 * 1024),
            name="ring_project",
        )(enc_out.reshape(block, d_model), norm_scale.reshape(1, d_model), w_key.reshape(n_layers, d_model, head_dim), w_value.reshape(n_layers, d_model, head_dim))
        side = jax.ShapeDtypeStruct((n_layers, n * block, head_dim), jnp.bfloat16)
        keys, values = pl.pallas_call(
            functools.partial(place_body, n, block),
            out_shape=(side, side),
            in_specs=[in_vmem],
            out_specs=(anywhere, anywhere),
            scratch_shapes=[pltpu.SemaphoreType.DMA((8 * (hops + 1),))],
            compiler_params=pltpu.CompilerParams(vmem_limit_bytes=4 * 1024 * 1024),
            name="place",
        )(res)
        shape = (n_layers, 1, n * block, 1, head_dim)
        return keys.reshape(shape), values.reshape(shape)

    weight_spec = P(None, None, "tp", None)
    cache_spec = P(None, "dp", None, "tp", None)
    return jax.shard_map(per_device, mesh=mesh, in_specs=(P("dp", "tp", None), P(None), weight_spec, weight_spec), out_specs=(cache_spec, cache_spec), check_vma=False)
```

```python
import functools

import jax
import jax.numpy as jnp
from jax import lax
from jax.experimental import pallas as pl
from jax.experimental.pallas import tpu as pltpu
from jax.sharding import PartitionSpec as P

NORM_EPS = 1e-6
MESH = pl.DeviceIdType.MESH
NORM_ROWS = 16
PIECES = 4


def ring_body(n, x_hbm, scale_ref, wk_hbm, wv_hbm, out, last, weights, acts, tokens, in_sem, w_sem, cw_send, cw_recv, ccw_send, ccw_recv, mate_send, mate_recv):
    me = lax.axis_index("tp")
    mate = me + 1 - 2 * lax.rem(me, 2)
    after = lax.rem(me + 2, n)
    before = lax.rem(me + n - 2, n)
    block, d_model = acts.shape
    piece = block // PIECES
    n_layers, _, both = weights.shape
    head_dim = both // 2
    arrivals = (n // 2 - 1) * PIECES // 2

    x_copies = []
    for part in (0, 2, 1, 3):
        rows = pl.ds(part * piece, piece)
        x_copies.append(pltpu.make_async_copy(x_hbm.at[rows], acts.at[rows], in_sem.at[part]))
        x_copies[-1].start()
    barrier = pltpu.get_barrier_semaphore()
    for other in (after, before, mate):
        pl.semaphore_signal(barrier, inc=1, device_id={"tp": other}, device_id_type=MESH)
    scale = scale_ref[...].reshape(1, d_model).astype(jnp.float32)

    def load_weights(layer):
        for side, src in enumerate((wk_hbm, wv_hbm)):
            yield pltpu.make_async_copy(src.at[layer], weights.at[layer, :, pl.ds(side * head_dim, head_dim)], w_sem.at[2 * layer + side])

    def normalize(part):
        @pl.loop(0, piece // NORM_ROWS)
        def _(i):
            rows = pl.ds(pl.multiple_of(part * piece + i * NORM_ROWS, NORM_ROWS), NORM_ROWS)
            x = acts[rows, :].astype(jnp.float32)
            mean_sq = jnp.mean(x * x, axis=-1, keepdims=True)
            tokens[0, rows, :] = (x * lax.rsqrt(mean_sq + NORM_EPS) * scale).astype(jnp.bfloat16)

    sends = []
    waits = {}

    def send(name, src, dst, send_sem, recv_sem, other):
        copy = pltpu.make_async_remote_copy(src_ref=src, dst_ref=dst, send_sem=send_sem, recv_sem=recv_sem, device_id={"tp": other}, device_id_type=MESH)
        copy.start()
        sends.append(copy)
        waits[name] = copy

    def landing(j):
        return last if j == arrivals - 1 else tokens.at[j + 2]

    def send_ring(j):
        for side, (send_sem, recv_sem, other) in enumerate(((cw_send, cw_recv, after), (ccw_send, ccw_recv, before))):
            if j < PIECES:
                own = (j + side * PIECES // 2) % PIECES
                src = tokens.at[0, pl.ds(own * piece, piece)]
            else:
                src = landing(j - PIECES).at[pl.ds(side * piece, piece)]
            send((side, j), src, landing(j).at[pl.ds(side * piece, piece)], send_sem.at[j], recv_sem.at[j], other)

    def handle(j):
        waits[0, j].wait_recv()
        waits[1, j].wait_recv()
        if j + PIECES < arrivals:
            send_ring(j + PIECES)
        here = landing(j)
        send((2, j), here.at[pl.ds(0, block // 2)], here.at[pl.ds(block // 2, block // 2)], mate_send.at[j + 1], mate_recv.at[j + 1], mate)

    def swapped(j):
        waits[2, j].wait_recv()

    def project(step, count, layer):
        rows = tokens[pl.ds(step, count)].reshape(count * block, d_model)
        both_sides = jnp.dot(rows, weights[layer], preferred_element_type=jnp.float32).astype(jnp.bfloat16)
        for i in range(count):
            out[step + i, layer] = both_sides[i * block : (i + 1) * block]

    x_copies[0].wait()
    x_copies[1].wait()
    for layer in range(n_layers):
        for copy in load_weights(layer):
            copy.start()
    normalize(0)
    normalize(2)
    pl.semaphore_wait(barrier, 3)
    send_ring(0)
    x_copies[2].wait()
    x_copies[3].wait()
    normalize(1)
    normalize(3)
    for j in range(1, PIECES):
        send_ring(j)
    send((2, -1), tokens.at[0], tokens.at[1], mate_send.at[0], mate_recv.at[0], mate)
    swapped(-1)

    @pl.loop(0, n_layers)
    def _(layer):
        for copy in load_weights(layer):
            copy.wait()
        project(0, 2, layer)

    late = arrivals - 6
    for j in range(0, late, 2):
        handle(j)
        handle(j + 1)
        swapped(j)
        swapped(j + 1)

        @pl.loop(0, n_layers)
        def _(layer):
            project(j + 2, 2, layer)

    handle(late)
    handle(late + 1)
    swapped(late)
    swapped(late + 1)
    for layer in range(n_layers):
        project(late + 2, 2, layer)
        if layer == n_layers // 2:
            handle(late + 2)
    swapped(late + 2)
    for layer in range(n_layers):
        project(late + 4, 1, layer)
        if layer == n_layers - 2:
            handle(late + 3)
    swapped(late + 3)
    for layer in range(n_layers):
        project(late + 5, 1, layer)
    handle(late + 4)
    swapped(late + 4)
    for layer in range(n_layers):
        project(late + 6, 1, layer)
    handle(late + 5)
    swapped(late + 5)
    for copy in sends:
        copy.wait_send()


def place_body(n, res, last, weights, k_hbm, v_hbm, tail, sem):
    me = lax.axis_index("tp")
    mate = me + 1 - 2 * lax.rem(me, 2)
    steps, n_layers, block, both = res.shape
    head_dim = both // 2
    piece = block // PIECES
    copies = []

    def put(src, rows):
        for side, dst in enumerate((k_hbm, v_hbm)):
            copy = pltpu.make_async_copy(src.at[:, :, pl.ds(side * head_dim, head_dim)], dst.at[:, rows, :], sem.at[len(copies)])
            copy.start()
            copies.append(copy)

    def put_arrival(src, j):
        away = 2 + 2 * (j // PIECES)
        for group in range(4):
            who = me if group < 2 else mate
            if group % 2 == 0:
                start = lax.rem(who + n - away, n) * block + (j % PIECES) * piece
            else:
                start = lax.rem(who + away, n) * block + ((j + PIECES // 2) % PIECES) * piece
            put(src.at[:, pl.ds(group * piece, piece)], pl.ds(pl.multiple_of(start, piece), piece))

    put(res.at[0], pl.ds(pl.multiple_of(me * block, block), block))
    put(res.at[1], pl.ds(pl.multiple_of(mate * block, block), block))
    for step in range(2, steps):
        put_arrival(res.at[step], step - 2)
    for layer in range(n_layers):
        tail[layer] = jnp.dot(last[...], weights[layer], preferred_element_type=jnp.float32).astype(jnp.bfloat16)
    put_arrival(tail, steps - 2)
    for copy in copies:
        copy.wait()


def solution(mesh):
    n = mesh.shape["tp"]

    def per_device(enc_out, norm_scale, w_key, w_value):
        _, block, d_model = enc_out.shape
        n_layers, _, _, head_dim = w_key.shape
        arrivals = (n // 2 - 1) * PIECES // 2
        anywhere = pl.BlockSpec(memory_space=pl.ANY)
        in_vmem = pl.BlockSpec(memory_space=pltpu.VMEM)
        res, last, weights = pl.pallas_call(
            functools.partial(ring_body, n),
            out_shape=(
                pltpu.VMEM((arrivals + 1, n_layers, block, 2 * head_dim), jnp.bfloat16),
                pltpu.VMEM((block, d_model), jnp.bfloat16),
                pltpu.VMEM((n_layers, d_model, 2 * head_dim), jnp.bfloat16),
            ),
            in_specs=[anywhere, in_vmem, anywhere, anywhere],
            out_specs=(in_vmem, in_vmem, in_vmem),
            scratch_shapes=[
                pltpu.VMEM((block, d_model), jnp.bfloat16),
                pltpu.VMEM((arrivals + 1, block, d_model), jnp.bfloat16),
                pltpu.SemaphoreType.DMA((PIECES,)),
                pltpu.SemaphoreType.DMA((2 * n_layers,)),
                pltpu.SemaphoreType.DMA((arrivals,)),
                pltpu.SemaphoreType.DMA((arrivals,)),
                pltpu.SemaphoreType.DMA((arrivals,)),
                pltpu.SemaphoreType.DMA((arrivals,)),
                pltpu.SemaphoreType.DMA((arrivals + 1,)),
                pltpu.SemaphoreType.DMA((arrivals + 1,)),
            ],
            compiler_params=pltpu.CompilerParams(collective_id=0, has_side_effects=True, vmem_limit_bytes=22 * 1024 * 1024),
            name="ring_project",
        )(enc_out.reshape(block, d_model), norm_scale, w_key.reshape(n_layers, d_model, head_dim), w_value.reshape(n_layers, d_model, head_dim))
        side = jax.ShapeDtypeStruct((n_layers, n * block, head_dim), jnp.bfloat16)
        keys, values = pl.pallas_call(
            functools.partial(place_body, n),
            out_shape=(side, side),
            in_specs=[in_vmem, in_vmem, in_vmem],
            out_specs=(anywhere, anywhere),
            scratch_shapes=[
                pltpu.VMEM((n_layers, block, 2 * head_dim), jnp.bfloat16),
                pltpu.SemaphoreType.DMA((4 + 8 * arrivals,)),
            ],
            compiler_params=pltpu.CompilerParams(vmem_limit_bytes=4 * 1024 * 1024),
            name="place",
        )(res, last, weights)
        shape = (n_layers, 1, n * block, 1, head_dim)
        return keys.reshape(shape), values.reshape(shape)

    weight_spec = P(None, None, "tp", None)
    cache_spec = P(None, "dp", None, "tp", None)
    return jax.shard_map(per_device, mesh=mesh, in_specs=(P("dp", "tp", None), P(None), weight_spec, weight_spec), out_specs=(cache_spec, cache_spec), check_vma=False)
```

```python
import functools

import jax
import jax.numpy as jnp
from jax import lax
from jax.experimental import pallas as pl
from jax.experimental.pallas import tpu as pltpu
from jax.sharding import PartitionSpec as P

NORM_EPS = 1e-6
MESH = pl.DeviceIdType.MESH
NORM_ROWS = 16
PIECES = 4
CUTS = 4


def token_starts(n, block, step):
    me = lax.axis_index("tp")
    mate = me + 1 - 2 * lax.rem(me, 2)
    piece = block // PIECES
    starts = []
    for group in range(4):
        if step < 2:
            start = (mate if step else me) * block + group * piece
        else:
            away = 2 + 2 * ((step - 2) // PIECES)
            who = me if group < 2 else mate
            owner = lax.rem(who + away, n) if group % 2 else lax.rem(who + n - away, n)
            start = owner * block + (step - 2 + group % 2 * PIECES // 2) % PIECES * piece
        starts.append(pl.multiple_of(start, piece))
    return starts


def ring_body(n, x_hbm, scale_ref, wk_hbm, wv_hbm, out, last, weights, acts, tokens, in_sem, w_sem, cw_send, cw_recv, ccw_send, ccw_recv, mate_send, mate_recv):
    me = lax.axis_index("tp")
    mate = me + 1 - 2 * lax.rem(me, 2)
    after = lax.rem(me + 2, n)
    before = lax.rem(me + n - 2, n)
    block, d_model = acts.shape
    piece = block // PIECES
    n_layers, _, both = weights.shape
    head_dim = both // 2
    arrivals = (n // 2 - 1) * PIECES // 2

    x_copies = []
    for part in (0, 2, 1, 3):
        rows = pl.ds(part * piece, piece)
        x_copies.append(pltpu.make_async_copy(x_hbm.at[rows], acts.at[rows], in_sem.at[part]))
        x_copies[-1].start()
    barrier = pltpu.get_barrier_semaphore()
    for other in (after, before, mate):
        pl.semaphore_signal(barrier, inc=1, device_id={"tp": other}, device_id_type=MESH)
    scale = scale_ref[...].reshape(1, d_model).astype(jnp.float32)

    def load_weights(layer):
        for side, src in enumerate((wk_hbm, wv_hbm)):
            yield pltpu.make_async_copy(src.at[layer], weights.at[layer, :, pl.ds(side * head_dim, head_dim)], w_sem.at[2 * layer + side])

    def normalize(part):
        @pl.loop(0, piece // NORM_ROWS)
        def _(i):
            rows = pl.ds(pl.multiple_of(part * piece + i * NORM_ROWS, NORM_ROWS), NORM_ROWS)
            x = acts[rows, :].astype(jnp.float32)
            mean_sq = jnp.mean(x * x, axis=-1, keepdims=True)
            tokens[0, rows, :] = (x * lax.rsqrt(mean_sq + NORM_EPS) * scale).astype(jnp.bfloat16)

    sends = []
    waits = {}

    def send(name, src, dst, send_sem, recv_sem, other):
        copy = pltpu.make_async_remote_copy(src_ref=src, dst_ref=dst, send_sem=send_sem, recv_sem=recv_sem, device_id={"tp": other}, device_id_type=MESH)
        copy.start()
        sends.append(copy)
        waits[name] = copy

    def landing(j):
        return last if j == arrivals - 1 else tokens.at[j + 2]

    def send_ring(j):
        cuts = CUTS if j == arrivals - 1 else 1
        for side, (send_sem, recv_sem, other) in enumerate(((cw_send, cw_recv, after), (ccw_send, ccw_recv, before))):
            if j < PIECES:
                own = (j + side * PIECES // 2) % PIECES
                src = tokens.at[0, pl.ds(own * piece, piece)]
            else:
                src = landing(j - PIECES).at[pl.ds(side * piece, piece)]
            dst = landing(j).at[pl.ds(side * piece, piece)]
            for cut in range(cuts):
                columns = pl.ds(cut * d_model // cuts, d_model // cuts)
                send((side, j, cut), src.at[:, columns], dst.at[:, columns], send_sem.at[j + cut], recv_sem.at[j + cut], other)

    def handle(j, cut=0):
        waits[0, j, cut].wait_recv()
        waits[1, j, cut].wait_recv()
        if j + PIECES < arrivals:
            send_ring(j + PIECES)
        cuts = CUTS if j == arrivals - 1 else 1
        here = landing(j).at[:, pl.ds(cut * d_model // cuts, d_model // cuts)]
        send((2, j, cut), here.at[pl.ds(0, block // 2)], here.at[pl.ds(block // 2, block // 2)], mate_send.at[j + cut + 1], mate_recv.at[j + cut + 1], mate)

    def swapped(j, cut=0):
        waits[2, j, cut].wait_recv()

    def project(step, count, layer):
        rows = tokens[pl.ds(step, count)].reshape(count * block, d_model)
        both_sides = jnp.dot(rows, weights[layer], preferred_element_type=jnp.float32).astype(jnp.bfloat16)
        for i in range(count):
            for group, start in enumerate(token_starts(n, block, step + i)):
                first = i * block + group * piece
                for side in range(2):
                    out[side, layer, pl.ds(start, piece)] = both_sides[first : first + piece, side * head_dim : (side + 1) * head_dim]

    x_copies[0].wait()
    x_copies[1].wait()
    for layer in range(n_layers):
        for copy in load_weights(layer):
            copy.start()
    normalize(0)
    normalize(2)
    pl.semaphore_wait(barrier, 3)
    send_ring(0)
    x_copies[2].wait()
    x_copies[3].wait()
    normalize(1)
    normalize(3)
    for j in range(1, PIECES):
        send_ring(j)
    send((2, -1, 0), tokens.at[0], tokens.at[1], mate_send.at[0], mate_recv.at[0], mate)
    swapped(-1)

    @pl.loop(0, n_layers)
    def _(layer):
        for copy in load_weights(layer):
            copy.wait()
        project(0, 2, layer)

    def project_pair(j, first, stop):
        loops = (stop - first) // 2

        @pl.loop(0, loops)
        def _(i):
            project(j + 2, 2, first + 2 * i)
            project(j + 2, 2, first + 2 * i + 1)

        for layer in range(first + 2 * loops, stop):
            project(j + 2, 2, layer)

    end = arrivals - 1
    handle(0)
    handle(1)
    for j in range(2, end - 5, 2):
        handle(j)
        swapped(j - 2)
        swapped(j - 1)
        project_pair(j - 2, 0, n_layers)
        handle(j + 1)
    handle(end - 5)
    swapped(end - 7)
    swapped(end - 6)
    project_pair(end - 7, 0, n_layers - 1)
    handle(end - 4)
    project_pair(end - 7, n_layers - 1, n_layers)
    swapped(end - 5)
    swapped(end - 4)
    project_pair(end - 5, 0, n_layers // 2)
    handle(end - 3)
    project_pair(end - 5, n_layers // 2, n_layers)
    swapped(end - 3)
    for layer in range(n_layers):
        if layer == 2:
            handle(end - 2)
        project(end - 1, 1, layer)
    swapped(end - 2)
    for layer in range(n_layers):
        project(end, 1, layer)
    handle(end - 1)
    swapped(end - 1)
    after_layer = {1: (0, 1), 2: (2,), 3: (3,)}
    for layer in range(n_layers):
        project(end + 1, 1, layer)
        for cut in after_layer.get(layer, ()):
            handle(end, cut)
    for cut in range(CUTS):
        swapped(end, cut)
    for copy in sends:
        copy.wait_send()


def place_body(n, res, last, weights, k_hbm, v_hbm, tail, sem):
    me = lax.axis_index("tp")
    _, n_layers, _, head_dim = res.shape
    block = last.shape[0]
    piece = block // PIECES
    steps = (n // 2 - 1) * PIECES // 2 + 2
    copies = []

    def put(src, side, rows, layers=slice(None)):
        copy = pltpu.make_async_copy(src, (k_hbm, v_hbm)[side].at[layers, rows], sem.at[len(copies)])
        copy.start()
        copies.append(copy)

    chip = me // 2
    for away in range(n // 2):
        if away != n // 4:
            rows = pl.ds(pl.multiple_of(lax.rem(chip + away, n // 2) * 2 * block, 2 * block), 2 * block)
            for side in range(2):
                put(res.at[side, :, rows], side, rows)
    for start in token_starts(n, block, steps - 2):
        rows = pl.ds(start, piece)
        for side in range(2):
            put(res.at[side, :, rows], side, rows)
    for layer in range(n_layers):
        tail[layer] = jnp.dot(last[...], weights[layer], preferred_element_type=jnp.float32).astype(jnp.bfloat16)
        for group, start in enumerate(token_starts(n, block, steps - 1)):
            for side in range(2):
                put(tail.at[pl.ds(layer, 1), pl.ds(group * piece, piece), pl.ds(side * head_dim, head_dim)], side, pl.ds(start, piece), pl.ds(layer, 1))
    for copy in copies:
        copy.wait()


def solution(mesh):
    n = mesh.shape["tp"]

    def per_device(enc_out, norm_scale, w_key, w_value):
        _, block, d_model = enc_out.shape
        n_layers, _, _, head_dim = w_key.shape
        arrivals = (n // 2 - 1) * PIECES // 2
        anywhere = pl.BlockSpec(memory_space=pl.ANY)
        in_vmem = pl.BlockSpec(memory_space=pltpu.VMEM)
        res, last, weights = pl.pallas_call(
            functools.partial(ring_body, n),
            out_shape=(
                pltpu.VMEM((2, n_layers, n * block, head_dim), jnp.bfloat16),
                pltpu.VMEM((block, d_model), jnp.bfloat16),
                pltpu.VMEM((n_layers, d_model, 2 * head_dim), jnp.bfloat16),
            ),
            in_specs=[anywhere, in_vmem, anywhere, anywhere],
            out_specs=(in_vmem, in_vmem, in_vmem),
            scratch_shapes=[
                pltpu.VMEM((block, d_model), jnp.bfloat16),
                pltpu.VMEM((arrivals + 1, block, d_model), jnp.bfloat16),
                pltpu.SemaphoreType.DMA((PIECES,)),
                pltpu.SemaphoreType.DMA((2 * n_layers,)),
                pltpu.SemaphoreType.DMA((arrivals + CUTS - 1,)),
                pltpu.SemaphoreType.DMA((arrivals + CUTS - 1,)),
                pltpu.SemaphoreType.DMA((arrivals + CUTS - 1,)),
                pltpu.SemaphoreType.DMA((arrivals + CUTS - 1,)),
                pltpu.SemaphoreType.DMA((arrivals + CUTS,)),
                pltpu.SemaphoreType.DMA((arrivals + CUTS,)),
            ],
            compiler_params=pltpu.CompilerParams(collective_id=0, has_side_effects=True, vmem_limit_bytes=22 * 1024 * 1024),
            name="ring_project",
        )(enc_out.reshape(block, d_model), norm_scale, w_key.reshape(n_layers, d_model, head_dim), w_value.reshape(n_layers, d_model, head_dim))
        side = jax.ShapeDtypeStruct((n_layers, n * block, head_dim), jnp.bfloat16)
        keys, values = pl.pallas_call(
            functools.partial(place_body, n),
            out_shape=(side, side),
            in_specs=[in_vmem, in_vmem, in_vmem],
            out_specs=(anywhere, anywhere),
            scratch_shapes=[
                pltpu.VMEM((n_layers, block, 2 * head_dim), jnp.bfloat16),
                pltpu.SemaphoreType.DMA((n + 6 + 8 * n_layers,)),
            ],
            compiler_params=pltpu.CompilerParams(vmem_limit_bytes=4 * 1024 * 1024),
            name="place",
        )(res, last, weights)
        shape = (n_layers, 1, n * block, 1, head_dim)
        return keys.reshape(shape), values.reshape(shape)

    weight_spec = P(None, None, "tp", None)
    cache_spec = P(None, "dp", None, "tp", None)
    return jax.shard_map(per_device, mesh=mesh, in_specs=(P("dp", "tp", None), P(None), weight_spec, weight_spec), out_specs=(cache_spec, cache_spec), check_vma=False)
```

```python
import functools

import jax
import jax.numpy as jnp
from jax import lax
from jax.experimental import pallas as pl
from jax.experimental.pallas import tpu as pltpu
from jax.sharding import PartitionSpec as P

NORM_EPS = 1e-6
MESH = pl.DeviceIdType.MESH
NORM_ROWS = 16
PIECES = 4
OPENING = 2
CUTS = 4


def token_starts(n, block, step):
    me = lax.axis_index("tp")
    mate = me + 1 - 2 * lax.rem(me, 2)
    piece = block // PIECES
    starts = []
    for group in range(4):
        if step < 2:
            start = (mate if step else me) * block + group * piece
        else:
            away = 2 + 2 * ((step - 2) // PIECES)
            who = me if group < 2 else mate
            owner = lax.rem(who + away, n) if group % 2 else lax.rem(who + n - away, n)
            start = owner * block + (step - 2 + group % 2 * PIECES // 2) % PIECES * piece
        starts.append(pl.multiple_of(start, piece))
    return starts


def ring_body(n, x_hbm, scale_hbm, wk_hbm, wv_hbm, out, last, weights, acts, scale_ref, tokens, in_sem, w_sem, cw_send, cw_recv, ccw_send, ccw_recv, mate_send, mate_recv):
    me = lax.axis_index("tp")
    mate = me + 1 - 2 * lax.rem(me, 2)
    after = lax.rem(me + 2, n)
    before = lax.rem(me + n - 2, n)
    block, d_model = acts.shape
    piece = block // PIECES
    n_layers, _, both = weights.shape
    head_dim = both // 2
    arrivals = (n // 2 - 1) * PIECES // 2

    scale_copy = pltpu.make_async_copy(scale_hbm, scale_ref, in_sem.at[PIECES])
    scale_copy.start()
    x_copies = []
    for part in (0, 2, 1, 3):
        rows = pl.ds(part * piece, piece)
        x_copies.append(pltpu.make_async_copy(x_hbm.at[rows], acts.at[rows], in_sem.at[part]))
        x_copies[-1].start()
    barrier = pltpu.get_barrier_semaphore()
    for other in (after, before, mate):
        pl.semaphore_signal(barrier, inc=1, device_id={"tp": other}, device_id_type=MESH)
    def load_weights(layer):
        for side, src in enumerate((wk_hbm, wv_hbm)):
            yield pltpu.make_async_copy(src.at[layer], weights.at[layer, :, pl.ds(side * head_dim, head_dim)], w_sem.at[2 * layer + side])

    def normalize(start):
        rows = pl.ds(start, NORM_ROWS)
        x = acts[rows, :].astype(jnp.float32)
        scale = scale_ref[...].reshape(1, d_model).astype(jnp.float32)
        mean_sq = jnp.mean(x * x, axis=-1, keepdims=True)
        tokens[0, rows, :] = (x * lax.rsqrt(mean_sq + NORM_EPS) * scale).astype(jnp.bfloat16)

    sends = []
    waits = {}

    def send(name, src, dst, send_sem, recv_sem, other):
        copy = pltpu.make_async_remote_copy(src_ref=src, dst_ref=dst, send_sem=send_sem, recv_sem=recv_sem, device_id={"tp": other}, device_id_type=MESH)
        copy.start()
        sends.append(copy)
        waits[name] = copy

    def landing(j):
        return last if j == arrivals - 1 else tokens.at[j + 2]

    def send_ring(j):
        cuts = CUTS if j == arrivals - 1 else 1
        for side, (send_sem, recv_sem, other) in enumerate(((cw_send, cw_recv, after), (ccw_send, ccw_recv, before))):
            if j < PIECES:
                own = (j + side * PIECES // 2) % PIECES
                src = tokens.at[0, pl.ds(own * piece, piece)]
            else:
                src = landing(j - PIECES).at[pl.ds(side * piece, piece)]
            dst = landing(j).at[pl.ds(side * piece, piece)]
            for cut in range(cuts):
                columns = pl.ds(cut * d_model // cuts, d_model // cuts)
                at = j + cut + OPENING - 1
                send((side, j, cut), src.at[:, columns], dst.at[:, columns], send_sem.at[at], recv_sem.at[at], other)

    def send_opening(cut):
        size = piece // OPENING
        for side, (send_sem, recv_sem, other) in enumerate(((cw_send, cw_recv, after), (ccw_send, ccw_recv, before))):
            src = tokens.at[0, pl.ds(side * (PIECES // 2) * piece + cut * size, size)]
            send((side, 0, cut), src, landing(0).at[pl.ds(side * piece + cut * size, size)], send_sem.at[cut], recv_sem.at[cut], other)

    def handle(j, cut=0):
        for part in range(OPENING) if j == 0 else (cut,):
            waits[0, j, part].wait_recv()
            waits[1, j, part].wait_recv()
        if j + PIECES < arrivals:
            send_ring(j + PIECES)
        cuts = CUTS if j == arrivals - 1 else 1
        here = landing(j).at[:, pl.ds(cut * d_model // cuts, d_model // cuts)]
        send((2, j, cut), here.at[pl.ds(0, block // 2)], here.at[pl.ds(block // 2, block // 2)], mate_send.at[j + cut + 1], mate_recv.at[j + cut + 1], mate)

    def swapped(j, cut=0):
        waits[2, j, cut].wait_recv()

    def project(step, count, layer):
        rows = tokens[pl.ds(step, count)].reshape(count * block, d_model)
        both_sides = jnp.dot(rows, weights[layer], preferred_element_type=jnp.float32).astype(jnp.bfloat16)
        for i in range(count):
            for group, start in enumerate(token_starts(n, block, step + i)):
                first = i * block + group * piece
                for side in range(2):
                    out[side, layer, pl.ds(start, piece)] = both_sides[first : first + piece, side * head_dim : (side + 1) * head_dim]

    scale_copy.wait()
    x_copies[0].wait()
    x_copies[1].wait()
    for layer in range(n_layers):
        for copy in load_weights(layer):
            copy.start()
    for cut in range(OPENING):
        for side in range(2):
            for start in range(0, piece // OPENING, NORM_ROWS):
                normalize((side * (PIECES // 2) * OPENING + cut) * (piece // OPENING) + start)
        if cut == 0:
            pl.semaphore_wait(barrier, 3)
        send_opening(cut)
    x_copies[2].wait()
    x_copies[3].wait()
    for part in (1, 3):
        for start in range(0, piece, NORM_ROWS):
            normalize(part * piece + start)
    for j in range(1, PIECES):
        send_ring(j)
    send((2, -1, 0), tokens.at[0], tokens.at[1], mate_send.at[0], mate_recv.at[0], mate)
    swapped(-1)

    @pl.loop(0, n_layers)
    def _(layer):
        for copy in load_weights(layer):
            copy.wait()
        project(0, 2, layer)

    def project_pair(j, first, stop):
        loops = (stop - first) // 2

        @pl.loop(0, loops)
        def _(i):
            project(j + 2, 2, first + 2 * i)
            project(j + 2, 2, first + 2 * i + 1)

        for layer in range(first + 2 * loops, stop):
            project(j + 2, 2, layer)

    end = arrivals - 1
    handle(0)
    handle(1)
    for j in range(2, end - 5, 2):
        handle(j)
        swapped(j - 2)
        swapped(j - 1)
        project_pair(j - 2, 0, n_layers)
        handle(j + 1)
    handle(end - 5)
    swapped(end - 7)
    swapped(end - 6)
    project_pair(end - 7, 0, n_layers - 1)
    handle(end - 4)
    project_pair(end - 7, n_layers - 1, n_layers)
    swapped(end - 5)
    swapped(end - 4)
    project_pair(end - 5, 0, n_layers // 2)
    handle(end - 3)
    project_pair(end - 5, n_layers // 2, n_layers)
    swapped(end - 3)
    for layer in range(n_layers):
        if layer == 2:
            handle(end - 2)
        project(end - 1, 1, layer)
    swapped(end - 2)
    for layer in range(n_layers):
        project(end, 1, layer)
    handle(end - 1)
    swapped(end - 1)
    after_layer = {1: (0, 1), 2: (2,), 3: (3,)}
    for layer in range(n_layers):
        project(end + 1, 1, layer)
        for cut in after_layer.get(layer, ()):
            handle(end, cut)
    for cut in range(CUTS):
        swapped(end, cut)
    for copy in sends:
        copy.wait_send()


def place_body(n, res, last, weights, k_hbm, v_hbm, tail, sem):
    me = lax.axis_index("tp")
    _, n_layers, _, head_dim = res.shape
    block = last.shape[0]
    piece = block // PIECES
    steps = (n // 2 - 1) * PIECES // 2 + 2
    copies = []

    def put(src, side, rows, layers=slice(None)):
        copy = pltpu.make_async_copy(src, (k_hbm, v_hbm)[side].at[layers, rows], sem.at[len(copies)])
        copy.start()
        copies.append(copy)

    chip = me // 2
    for away in range(n // 2):
        if away != n // 4:
            rows = pl.ds(pl.multiple_of(lax.rem(chip + away, n // 2) * 2 * block, 2 * block), 2 * block)
            for side in range(2):
                put(res.at[side, :, rows], side, rows)
    for start in token_starts(n, block, steps - 2):
        rows = pl.ds(start, piece)
        for side in range(2):
            put(res.at[side, :, rows], side, rows)
    for layer in range(n_layers):
        tail[layer] = jnp.dot(last[...], weights[layer], preferred_element_type=jnp.float32).astype(jnp.bfloat16)
        for group, start in enumerate(token_starts(n, block, steps - 1)):
            for side in range(2):
                put(tail.at[pl.ds(layer, 1), pl.ds(group * piece, piece), pl.ds(side * head_dim, head_dim)], side, pl.ds(start, piece), pl.ds(layer, 1))
    for copy in copies:
        copy.wait()


def solution(mesh):
    n = mesh.shape["tp"]

    def per_device(enc_out, norm_scale, w_key, w_value):
        _, block, d_model = enc_out.shape
        n_layers, _, _, head_dim = w_key.shape
        arrivals = (n // 2 - 1) * PIECES // 2
        anywhere = pl.BlockSpec(memory_space=pl.ANY)
        in_vmem = pl.BlockSpec(memory_space=pltpu.VMEM)
        res, last, weights = pl.pallas_call(
            functools.partial(ring_body, n),
            out_shape=(
                pltpu.VMEM((2, n_layers, n * block, head_dim), jnp.bfloat16),
                pltpu.VMEM((block, d_model), jnp.bfloat16),
                pltpu.VMEM((n_layers, d_model, 2 * head_dim), jnp.bfloat16),
            ),
            in_specs=[anywhere, anywhere, anywhere, anywhere],
            out_specs=(in_vmem, in_vmem, in_vmem),
            scratch_shapes=[
                pltpu.VMEM((block, d_model), jnp.bfloat16),
                pltpu.VMEM((d_model,), jnp.bfloat16),
                pltpu.VMEM((arrivals + 1, block, d_model), jnp.bfloat16),
                pltpu.SemaphoreType.DMA((PIECES + 1,)),
                pltpu.SemaphoreType.DMA((2 * n_layers,)),
                pltpu.SemaphoreType.DMA((arrivals + CUTS + OPENING - 2,)),
                pltpu.SemaphoreType.DMA((arrivals + CUTS + OPENING - 2,)),
                pltpu.SemaphoreType.DMA((arrivals + CUTS + OPENING - 2,)),
                pltpu.SemaphoreType.DMA((arrivals + CUTS + OPENING - 2,)),
                pltpu.SemaphoreType.DMA((arrivals + CUTS,)),
                pltpu.SemaphoreType.DMA((arrivals + CUTS,)),
            ],
            compiler_params=pltpu.CompilerParams(collective_id=0, has_side_effects=True, vmem_limit_bytes=22 * 1024 * 1024),
            name="ring_project",
        )(enc_out.reshape(block, d_model), norm_scale, w_key.reshape(n_layers, d_model, head_dim), w_value.reshape(n_layers, d_model, head_dim))
        side = jax.ShapeDtypeStruct((n_layers, n * block, head_dim), jnp.bfloat16)
        keys, values = pl.pallas_call(
            functools.partial(place_body, n),
            out_shape=(side, side),
            in_specs=[in_vmem, in_vmem, in_vmem],
            out_specs=(anywhere, anywhere),
            scratch_shapes=[
                pltpu.VMEM((n_layers, block, 2 * head_dim), jnp.bfloat16),
                pltpu.SemaphoreType.DMA((n + 6 + 8 * n_layers,)),
            ],
            compiler_params=pltpu.CompilerParams(vmem_limit_bytes=4 * 1024 * 1024),
            name="place",
        )(res, last, weights)
        shape = (n_layers, 1, n * block, 1, head_dim)
        return keys.reshape(shape), values.reshape(shape)

    weight_spec = P(None, None, "tp", None)
    cache_spec = P(None, "dp", None, "tp", None)
    return jax.shard_map(per_device, mesh=mesh, in_specs=(P("dp", "tp", None), P(None), weight_spec, weight_spec), out_specs=(cache_spec, cache_spec), check_vma=False)
```

```python
import functools

import jax
import jax.numpy as jnp
from jax import lax
from jax.experimental import pallas as pl
from jax.experimental.pallas import tpu as pltpu
from jax.sharding import PartitionSpec as P

NORM_EPS = 1e-6
MESH = pl.DeviceIdType.MESH
NORM_ROWS = 16
PIECES = 4
OPENING = 2
CUTS = 4


def token_starts(n, block, step):
    me = lax.axis_index("tp")
    mate = me + 1 - 2 * lax.rem(me, 2)
    piece = block // PIECES
    starts = []
    for group in range(4):
        if step < 2:
            start = (mate if step else me) * block + group * piece
        else:
            away = 2 + 2 * ((step - 2) // PIECES)
            who = me if group < 2 else mate
            owner = lax.rem(who + away, n) if group % 2 else lax.rem(who + n - away, n)
            start = owner * block + (step - 2 + group % 2 * PIECES // 2) % PIECES * piece
        starts.append(pl.multiple_of(start, piece))
    return starts


def ring_body(n, x_hbm, scale_hbm, wk_hbm, wv_hbm, out, last, weights, acts, scale_ref, tokens, in_sem, w_sem, cw_send, cw_recv, ccw_send, ccw_recv, mate_send, mate_recv):
    me = lax.axis_index("tp")
    mate = me + 1 - 2 * lax.rem(me, 2)
    after = lax.rem(me + 2, n)
    before = lax.rem(me + n - 2, n)
    block, d_model = acts.shape
    piece = block // PIECES
    n_layers, _, both = weights.shape
    head_dim = both // 2
    arrivals = (n // 2 - 1) * PIECES // 2

    scale_copy = pltpu.make_async_copy(scale_hbm, scale_ref, in_sem.at[PIECES])
    scale_copy.start()
    x_copies = []
    for part in (0, 2, 1, 3):
        rows = pl.ds(part * piece, piece)
        x_copies.append(pltpu.make_async_copy(x_hbm.at[rows], acts.at[rows], in_sem.at[part]))
        x_copies[-1].start()
    barrier = pltpu.get_barrier_semaphore()
    for other in (after, before, mate):
        pl.semaphore_signal(barrier, inc=1, device_id={"tp": other}, device_id_type=MESH)
    def load_weights(layer):
        for side, src in enumerate((wk_hbm, wv_hbm)):
            yield pltpu.make_async_copy(src.at[layer], weights.at[layer, :, pl.ds(side * head_dim, head_dim)], w_sem.at[2 * layer + side])

    def normalize(start):
        rows = pl.ds(start, NORM_ROWS)
        x = acts[rows, :].astype(jnp.float32)
        scale = scale_ref[...].reshape(1, d_model).astype(jnp.float32)
        mean_sq = jnp.mean(x * x, axis=-1, keepdims=True)
        tokens[0, rows, :] = (x * lax.rsqrt(mean_sq + NORM_EPS) * scale).astype(jnp.bfloat16)

    sends = []
    waits = {}

    def send(name, src, dst, send_sem, recv_sem, other):
        copy = pltpu.make_async_remote_copy(src_ref=src, dst_ref=dst, send_sem=send_sem, recv_sem=recv_sem, device_id={"tp": other}, device_id_type=MESH)
        copy.start()
        sends.append(copy)
        waits[name] = copy

    def landing(j):
        return last if j == arrivals - 1 else tokens.at[j + 2]

    def send_ring(j):
        cuts = CUTS if j == arrivals - 1 else 1
        for side, (send_sem, recv_sem, other) in enumerate(((cw_send, cw_recv, after), (ccw_send, ccw_recv, before))):
            if j < PIECES:
                own = (j + side * PIECES // 2) % PIECES
                src = tokens.at[0, pl.ds(own * piece, piece)]
            else:
                src = landing(j - PIECES).at[pl.ds(side * piece, piece)]
            dst = landing(j).at[pl.ds(side * piece, piece)]
            for cut in range(max(cuts - 1, 1)):
                columns = pl.ds(cut * d_model // cuts, d_model // cuts)
                at = j + cut + OPENING - 1
                send((side, j, cut), src.at[:, columns], dst.at[:, columns], send_sem.at[at], recv_sem.at[at], other)

    def send_opening(cut):
        size = piece // OPENING
        for side, (send_sem, recv_sem, other) in enumerate(((cw_send, cw_recv, after), (ccw_send, ccw_recv, before))):
            src = tokens.at[0, pl.ds(side * (PIECES // 2) * piece + cut * size, size)]
            send((side, 0, cut), src, landing(0).at[pl.ds(side * piece + cut * size, size)], send_sem.at[cut], recv_sem.at[cut], other)

    final = d_model // CUTS
    whole = pl.ds(d_model - final, final)
    kept = pl.ds(d_model - final, final // 2)
    lent = pl.ds(d_model - final // 2, final // 2)
    odd = lax.rem(me, 2) == 1
    even = lax.rem(me, 2) == 0

    def final_ring(lender, extra):
        copies = []
        for side, (send_sem, recv_sem, other) in enumerate(((cw_send, cw_recv, after), (ccw_send, ccw_recv, before))):
            rows = pl.ds(side * piece + (block // 2 if extra else 0), piece)
            columns = lent if extra else whole if lender else kept
            at = arrivals + CUTS + OPENING - 3 + extra
            copies.append(pltpu.make_async_remote_copy(src_ref=landing(arrivals - 1 - PIECES).at[rows, columns], dst_ref=last.at[rows, columns], send_sem=send_sem.at[at], recv_sem=recv_sem.at[at], device_id={"tp": other}, device_id_type=MESH))
        return copies

    def final_swap(lender):
        mine, other = pl.ds(0, block // 2), pl.ds(block // 2, block // 2)
        moves = [(mine, other, whole if lender else kept)] + ([(other, mine, lent)] if lender else [])
        at = arrivals + CUTS - 1
        return [pltpu.make_async_remote_copy(src_ref=last.at[src, columns], dst_ref=last.at[dst, columns], send_sem=mate_send.at[at + i], recv_sem=mate_recv.at[at + i], device_id={"tp": mate}, device_id_type=MESH) for i, (src, dst, columns) in enumerate(moves)]

    def each_core(act):
        pl.when(odd)(lambda: act(True))
        pl.when(even)(lambda: act(False))

    def final_send(lender):
        for copy in final_ring(lender, 0) + (final_ring(lender, 1) if lender else []):
            copy.start()

    def final_handle(lender):
        for copy in final_ring(lender, 0) + (final_ring(lender, 1) if lender else []):
            copy.wait_recv()
        for copy in final_swap(lender):
            copy.start()

    def final_swapped(lender):
        for copy in final_swap(not lender):
            copy.wait_recv()

    def final_sent(lender):
        for copy in final_ring(lender, 0) + (final_ring(lender, 1) if lender else []) + final_swap(lender):
            copy.wait_send()

    def handle(j, cut=0):
        for part in range(OPENING) if j == 0 else (cut,):
            waits[0, j, part].wait_recv()
            waits[1, j, part].wait_recv()
        if j + PIECES < arrivals:
            send_ring(j + PIECES)
        cuts = CUTS if j == arrivals - 1 else 1
        here = landing(j).at[:, pl.ds(cut * d_model // cuts, d_model // cuts)]
        send((2, j, cut), here.at[pl.ds(0, block // 2)], here.at[pl.ds(block // 2, block // 2)], mate_send.at[j + cut + 1], mate_recv.at[j + cut + 1], mate)

    def swapped(j, cut=0):
        waits[2, j, cut].wait_recv()

    def project(step, count, layer):
        rows = tokens[pl.ds(step, count)].reshape(count * block, d_model)
        both_sides = jnp.dot(rows, weights[layer], preferred_element_type=jnp.float32).astype(jnp.bfloat16)
        for i in range(count):
            for group, start in enumerate(token_starts(n, block, step + i)):
                first = i * block + group * piece
                for side in range(2):
                    out[side, layer, pl.ds(start, piece)] = both_sides[first : first + piece, side * head_dim : (side + 1) * head_dim]

    scale_copy.wait()
    x_copies[0].wait()
    x_copies[1].wait()
    for layer in range(n_layers):
        for copy in load_weights(layer):
            copy.start()
    for cut in range(OPENING):
        for side in range(2):
            for start in range(0, piece // OPENING, NORM_ROWS):
                normalize((side * (PIECES // 2) * OPENING + cut) * (piece // OPENING) + start)
        if cut == 0:
            pl.semaphore_wait(barrier, 3)
        send_opening(cut)
    x_copies[2].wait()
    x_copies[3].wait()
    for part in (1, 3):
        for start in range(0, piece, NORM_ROWS):
            normalize(part * piece + start)
    for j in range(1, PIECES):
        send_ring(j)
    send((2, -1, 0), tokens.at[0], tokens.at[1], mate_send.at[0], mate_recv.at[0], mate)
    swapped(-1)

    @pl.loop(0, n_layers)
    def _(layer):
        for copy in load_weights(layer):
            copy.wait()
        project(0, 2, layer)

    def project_pair(j, first, stop):
        loops = (stop - first) // 2

        @pl.loop(0, loops)
        def _(i):
            project(j + 2, 2, first + 2 * i)
            project(j + 2, 2, first + 2 * i + 1)

        for layer in range(first + 2 * loops, stop):
            project(j + 2, 2, layer)

    end = arrivals - 1
    handle(0)
    handle(1)
    for j in range(2, end - 5, 2):
        handle(j)
        swapped(j - 2)
        swapped(j - 1)
        project_pair(j - 2, 0, n_layers)
        handle(j + 1)
    handle(end - 5)
    swapped(end - 7)
    swapped(end - 6)
    project_pair(end - 7, 0, n_layers - 1)
    handle(end - 4)
    project_pair(end - 7, n_layers - 1, n_layers)
    swapped(end - 5)
    swapped(end - 4)
    each_core(final_send)
    project_pair(end - 5, 0, n_layers // 2)
    handle(end - 3)
    project_pair(end - 5, n_layers // 2, n_layers)
    swapped(end - 3)
    for layer in range(n_layers):
        if layer == 2:
            handle(end - 2)
        project(end - 1, 1, layer)
    swapped(end - 2)
    for layer in range(n_layers):
        project(end, 1, layer)
    handle(end - 1)
    swapped(end - 1)
    after_layer = {1: (0, 1), 2: (2,), 3: (3,)}
    for layer in range(n_layers):
        project(end + 1, 1, layer)
        for cut in after_layer.get(layer, ()):
            if cut < CUTS - 1:
                handle(end, cut)
            else:
                each_core(final_handle)
    for cut in range(CUTS - 1):
        swapped(end, cut)
    each_core(final_swapped)
    each_core(final_sent)
    for copy in sends:
        copy.wait_send()


def place_body(n, res, last, weights, k_hbm, v_hbm, tail, sem):
    me = lax.axis_index("tp")
    _, n_layers, _, head_dim = res.shape
    block = last.shape[0]
    piece = block // PIECES
    steps = (n // 2 - 1) * PIECES // 2 + 2
    copies = []

    def put(src, side, rows, layers=slice(None)):
        copy = pltpu.make_async_copy(src, (k_hbm, v_hbm)[side].at[layers, rows], sem.at[len(copies)])
        copy.start()
        copies.append(copy)

    chip = me // 2
    for away in range(n // 2):
        if away != n // 4:
            rows = pl.ds(pl.multiple_of(lax.rem(chip + away, n // 2) * 2 * block, 2 * block), 2 * block)
            for side in range(2):
                put(res.at[side, :, rows], side, rows)
    for start in token_starts(n, block, steps - 2):
        rows = pl.ds(start, piece)
        for side in range(2):
            put(res.at[side, :, rows], side, rows)
    for layer in range(n_layers):
        tail[layer] = jnp.dot(last[...], weights[layer], preferred_element_type=jnp.float32).astype(jnp.bfloat16)
        for group, start in enumerate(token_starts(n, block, steps - 1)):
            for side in range(2):
                put(tail.at[pl.ds(layer, 1), pl.ds(group * piece, piece), pl.ds(side * head_dim, head_dim)], side, pl.ds(start, piece), pl.ds(layer, 1))
    for copy in copies:
        copy.wait()


def solution(mesh):
    n = mesh.shape["tp"]

    def per_device(enc_out, norm_scale, w_key, w_value):
        _, block, d_model = enc_out.shape
        n_layers, _, _, head_dim = w_key.shape
        arrivals = (n // 2 - 1) * PIECES // 2
        anywhere = pl.BlockSpec(memory_space=pl.ANY)
        in_vmem = pl.BlockSpec(memory_space=pltpu.VMEM)
        res, last, weights = pl.pallas_call(
            functools.partial(ring_body, n),
            out_shape=(
                pltpu.VMEM((2, n_layers, n * block, head_dim), jnp.bfloat16),
                pltpu.VMEM((block, d_model), jnp.bfloat16),
                pltpu.VMEM((n_layers, d_model, 2 * head_dim), jnp.bfloat16),
            ),
            in_specs=[anywhere, anywhere, anywhere, anywhere],
            out_specs=(in_vmem, in_vmem, in_vmem),
            scratch_shapes=[
                pltpu.VMEM((block, d_model), jnp.bfloat16),
                pltpu.VMEM((d_model,), jnp.bfloat16),
                pltpu.VMEM((arrivals + 1, block, d_model), jnp.bfloat16),
                pltpu.SemaphoreType.DMA((PIECES + 1,)),
                pltpu.SemaphoreType.DMA((2 * n_layers,)),
                pltpu.SemaphoreType.DMA((arrivals + CUTS + OPENING - 1,)),
                pltpu.SemaphoreType.DMA((arrivals + CUTS + OPENING - 1,)),
                pltpu.SemaphoreType.DMA((arrivals + CUTS + OPENING - 1,)),
                pltpu.SemaphoreType.DMA((arrivals + CUTS + OPENING - 1,)),
                pltpu.SemaphoreType.DMA((arrivals + CUTS + 1,)),
                pltpu.SemaphoreType.DMA((arrivals + CUTS + 1,)),
            ],
            compiler_params=pltpu.CompilerParams(collective_id=0, has_side_effects=True, vmem_limit_bytes=22 * 1024 * 1024),
            name="ring_project",
        )(enc_out.reshape(block, d_model), norm_scale, w_key.reshape(n_layers, d_model, head_dim), w_value.reshape(n_layers, d_model, head_dim))
        side = jax.ShapeDtypeStruct((n_layers, n * block, head_dim), jnp.bfloat16)
        keys, values = pl.pallas_call(
            functools.partial(place_body, n),
            out_shape=(side, side),
            in_specs=[in_vmem, in_vmem, in_vmem],
            out_specs=(anywhere, anywhere),
            scratch_shapes=[
                pltpu.VMEM((n_layers, block, 2 * head_dim), jnp.bfloat16),
                pltpu.SemaphoreType.DMA((n + 6 + 8 * n_layers,)),
            ],
            compiler_params=pltpu.CompilerParams(vmem_limit_bytes=4 * 1024 * 1024),
            name="place",
        )(res, last, weights)
        shape = (n_layers, 1, n * block, 1, head_dim)
        return keys.reshape(shape), values.reshape(shape)

    weight_spec = P(None, None, "tp", None)
    cache_spec = P(None, "dp", None, "tp", None)
    return jax.shard_map(per_device, mesh=mesh, in_specs=(P("dp", "tp", None), P(None), weight_spec, weight_spec), out_specs=(cache_spec, cache_spec), check_vma=False)
```
